32 devices in a mesh: region: 4 (over z), depth: 2 (over y), member: 4 (over x, core).
Axes of the slice: x: 2, y: 2, z: 4, core: 2. Of those that a mesh axis runs over, the one named last changes fastest.
Arguments:
- ensemble: bfloat16 [14, 384, 4096], P('depth', 'member', 'region'), may hold values from -6 to 6
- obs_weights: float32 [14], P('depth'), may hold values from -1.5 to 1.5
- obs_tiles: int32 [2048], P('region'), may hold values from 0 to 1023
- obs_values: float32 [2048], P('region'), may hold values from -8 to 8
- obs_error: float32 [2048], P('region'), may hold values from 0.2 to 2
- obs_noise: float32 [384, 2048], P('member', 'region'), may hold values from -6 to 6
Outputs:
- analysis: bfloat16 [14, 384, 4096], P('depth', 'member', 'region')
- inflation: float32 [], replicated
The draws below stay inside these ranges and needn't reach their ends.
Inputs may be any that keep to these rules, and one draw needn't show every extreme that they name: `obs_tiles`: the tile of the observation, counted within the 1024 tiles of the region whose block holds the observation.
All inputs are finite; a program needn't handle non-finite values.
Results may differ from the reference program's by a relative error of at most 0.011.
Values may be sent and summed in bfloat16 or wider, within the bound.
A program may use at most 64 MiB of HBM per device.

```python
import math
import jax
import jax.numpy as jnp
from jax import lax

VARS = 14
MEMBERS = 384
TILE_DEV = 1024
OBS_DEV = 512
NTILES = 4096
NOBS = 2048
RADIUS = 1024
N_REGION = 4


def touch_ends(values, own_key, smallest, largest):
    shape = values.shape
    spot = [jax.random.randint(jax.random.fold_in(own_key, axis), (), 0, shape[axis]) for axis in range(len(shape))]
    values = values.at[tuple(spot)].set(smallest)
    longest = shape.index(max(shape))
    spot[longest] = (spot[longest] + 1) % shape[longest]
    return values.at[tuple(spot)].set(largest)


def block_levels(key, dims, cuts, least, top_value):
    level = 1.0
    for dim, blocks in cuts:
        draws = jax.random.uniform(jax.random.fold_in(jax.random.fold_in(key, 6), dim), (blocks,), jnp.float32, least / len(cuts), top_value / len(cuts))
        level = level * jnp.repeat(jnp.exp(draws), dims[dim] // blocks).reshape((-1,) + (1,) * (len(dims) - 1 - dim))
    return level


def gaussian(key, dims, scale, limit, split=(), kind=jnp.bfloat16):
    factor_of = block_levels(key, dims, split, -0.22, 0.18) if split else 1.0
    drawn = jax.random.normal(key, dims, jnp.float32) * scale * factor_of
    return jnp.minimum(jnp.maximum(drawn, -limit), limit).astype(kind)


def setup_inputs(seed: int = 0) -> dict:
    splits = jax.random.split(jax.random.key(seed), 7)
    return {
        "ensemble": gaussian(splits[0], (VARS, MEMBERS, NTILES), 1.0, 6.0, ((0, 2), (1, 4), (2, 4))),
        "obs_weights": gaussian(splits[1], (VARS,), VARS ** -0.5, 1.5, ((0, 2),), jnp.float32),
        "obs_tiles": touch_ends(jax.random.randint(splits[2], (NOBS,), 0, TILE_DEV), jax.random.fold_in(splits[2], 1), 0, TILE_DEV - 1).astype(jnp.int32),
        "obs_values": gaussian(splits[3], (NOBS,), 2.0, 8.0, ((0, 4),), jnp.float32),
        "obs_error": jnp.clip(jnp.exp(math.log(2.0) - 2.3025851 * jax.random.uniform(splits[4], (NOBS,), jnp.float32) ** block_levels(splits[4], (NOBS,), ((0, 4),), -0.2, 0.2)), 0.2, 2.0),
        "obs_noise": gaussian(splits[5], (MEMBERS, NOBS), 1.0, 6.0, ((0, 4), (1, 4)), jnp.float32),
    }


def reference(ensemble, obs_weights, obs_tiles, obs_values, obs_error, obs_noise):
    state_f = ensemble.astype(jnp.float32)
    state_mean = lax.optimization_barrier(jnp.sum(state_f, axis=1)) / MEMBERS
    anomalies = (state_f - state_mean[:, None, :]).astype(jnp.bfloat16)
    obs_region = jnp.arange(NOBS, dtype=jnp.int32) // OBS_DEV
    obs_global = obs_region * TILE_DEV + obs_tiles.astype(jnp.int32)
    picked = jnp.take(ensemble, obs_global, axis=2).astype(jnp.float32)
    predicted = jnp.einsum('lmk,l->mk', picked, obs_weights.astype(jnp.float32), precision=lax.Precision.HIGHEST)
    obs_mean = lax.optimization_barrier(jnp.sum(predicted, axis=0)) / MEMBERS
    obs_dev = predicted - obs_mean[None, :]
    obs_spread = lax.optimization_barrier(jnp.sum(obs_dev * obs_dev, axis=0)) / (MEMBERS - 1)
    innovation = obs_values - obs_mean
    inflation = jnp.sum(innovation * innovation) / jnp.sum(obs_spread + obs_error)
    infl_root = jnp.sqrt(inflation)
    factor = inflation / (inflation * obs_spread + obs_error)
    obs_anom = obs_dev.astype(jnp.bfloat16)
    perturbed = (innovation[None, :] + jnp.sqrt(obs_error)[None, :] * obs_noise - infl_root * obs_dev).astype(jnp.bfloat16)
    padded_anom = jnp.pad(obs_anom, ((0, 0), (OBS_DEV, OBS_DEV)))
    padded_pert = jnp.pad(perturbed, ((0, 0), (OBS_DEV, OBS_DEV)))
    padded_factor = jnp.pad(factor, (OBS_DEV, OBS_DEV))
    padded_pos = jnp.pad(obs_global.astype(jnp.float32), (OBS_DEV, OBS_DEV))

    def one_region(region_id):
        first_obs = region_id * OBS_DEV
        anom_window = lax.dynamic_slice_in_dim(padded_anom, first_obs, 3 * OBS_DEV, 1).astype(jnp.float32)
        pert_window = lax.dynamic_slice_in_dim(padded_pert, first_obs, 3 * OBS_DEV, 1).astype(jnp.float32)
        factor_window = lax.dynamic_slice_in_dim(padded_factor, first_obs, 3 * OBS_DEV, 0)
        pos_window = lax.dynamic_slice_in_dim(padded_pos, first_obs, 3 * OBS_DEV, 0)
        first_tile = region_id * TILE_DEV
        region_anom = lax.dynamic_slice_in_dim(anomalies, first_tile, TILE_DEV, 2).astype(jnp.float32)
        region_mean = lax.dynamic_slice_in_dim(state_mean, first_tile, TILE_DEV, 1)
        covariance = jnp.einsum('lmt,mj->ltj', region_anom, anom_window) / (MEMBERS - 1)
        tile_pos = (first_tile + jnp.arange(TILE_DEV, dtype=jnp.int32)).astype(jnp.float32)
        closeness = jnp.maximum(0.0, 1.0 - jnp.abs(tile_pos[:, None] - pos_window[None, :]) / RADIUS)
        kalman_gain = (covariance * (closeness * closeness * factor_window[None, :])[None]).astype(jnp.bfloat16)
        increment = jnp.einsum('ltj,mj->lmt', kalman_gain.astype(jnp.float32), pert_window)
        return (region_mean[:, None, :] + infl_root * region_anom + increment).astype(jnp.bfloat16)
    region_out = lax.map(one_region, jnp.arange(N_REGION, dtype=jnp.int32))
    analysis = jnp.transpose(region_out, (1, 2, 0, 3)).reshape(VARS, MEMBERS, NTILES)
    return (analysis, inflation)
```

```python
import functools

import jax
import jax.numpy as jnp
from jax import lax
from jax.experimental import pallas as pl
from jax.experimental.pallas import tpu as pltpu
from jax.sharding import PartitionSpec as P

RADIUS = 1024
F32 = jnp.float32
BF16 = jnp.bfloat16
MESH = pl.DeviceIdType.MESH


def kernel(
    sizes,
    weights,
    ensemble,
    tiles,
    values,
    errors,
    noise,
    out,
    infl_out,
    own,
    gathered,
    noise_v,
    part,
    part_in,
    sums,
    squares,
    totals,
    stats,
    obs,
    pert,
    obs_t,
    taper,
    anom,
    gain,
    result,
    local_sem,
    send_e,
    recv_e,
    send_s,
    recv_s,
    send_p,
    recv_p,
    send_q,
    recv_q,
    send_o,
    recv_o,
    send_g,
    recv_g,
    send_z,
    recv_z,
    send_st,
    recv_st,
    send_ps,
    recv_ps,
    send_pz,
    recv_pz,
    send_out,
    recv_out,
    own_out,
):
    nr, nd, nm, nl, mm, tt, kk = sizes
    ng = nm // 2
    half = tt // 2
    members = nm * mm
    r = lax.axis_index("region")
    d = lax.axis_index("depth")
    me = lax.axis_index("member")
    q = me // 2
    c = me % 2
    sib = 2 * q + (1 - c)
    has_side = (r > 0, r < nr - 1)

    def dev(region=None, depth=None, member=None):
        return {
            "region": r if region is None else region,
            "depth": d if depth is None else depth,
            "member": me if member is None else member,
        }

    def rdma(src, dst, ssem, rsem, device):
        return pltpu.make_async_remote_copy(
            src_ref=src,
            dst_ref=dst,
            send_sem=ssem,
            recv_sem=rsem,
            device_id=device,
            device_id_type=MESH,
        )

    local_own = pltpu.make_async_copy(ensemble, own, local_sem.at[0])
    local_own.start()
    local_half = pltpu.make_async_copy(
        ensemble.at[:, :, pl.ds(pl.multiple_of(c * half, 128), half)],
        gathered.at[:, me],
        local_sem.at[1],
    )
    local_half.start()
    local_noise = pltpu.make_async_copy(noise, noise_v, local_sem.at[2])
    local_noise.start()

    group = [(i, j) for i in range(nd) for j in range(nm) if i or j]
    barrier = pltpu.get_barrier_semaphore()
    signals = 0
    for i, j in group:
        pl.semaphore_signal(
            barrier,
            inc=1,
            device_id=dev(depth=(d + i) % nd, member=(me + j) % nm),
            device_id_type=MESH,
        )
        signals += 1
    for i in range(1, nr):
        pl.semaphore_signal(
            barrier, inc=1, device_id=dev(region=(r + i) % nr), device_id_type=MESH
        )
        signals += 1
    for i in (1, nr - 1):
        pl.semaphore_signal(
            barrier,
            inc=1,
            device_id=dev(region=(r + i) % nr, member=sib),
            device_id_type=MESH,
        )
        signals += 1
    pl.semaphore_wait(barrier, signals)

    def bulk(l, j):
        to = (me + j) % nm
        return rdma(
            ensemble.at[l, :, pl.ds(pl.multiple_of((to % 2) * half, 128), half)],
            gathered.at[l, me],
            send_e.at[l, j],
            recv_e.at[l, me],
            dev(member=to),
        )

    def send_bulk(l):
        for j in range(1, nm):
            bulk(l, j).start()

    send_bulk(0)

    local_own.wait()
    total = own[0].astype(F32) * weights[0]
    for l in range(1, nl):
        total = total + own[l].astype(F32) * weights[l]
    hi = total.astype(BF16)
    rest = total - hi.astype(F32)
    mid = rest.astype(BF16)
    low = (rest - mid.astype(F32)).astype(BF16)
    tile_ids = lax.broadcasted_iota(jnp.int32, (tt, kk), 0)
    onehot = jnp.where(tile_ids == tiles[...], 1.0, 0.0).astype(BF16)
    picked = (
        jnp.dot(hi, onehot, preferred_element_type=F32)
        + jnp.dot(mid, onehot, preferred_element_type=F32)
        + jnp.dot(low, onehot, preferred_element_type=F32)
    )
    part[...] = picked
    here = d * nm + me
    sums[here] = jnp.broadcast_to(jnp.sum(picked, axis=0, keepdims=True), (8, kk))

    def part_copy(i):
        to = (d + i) % nd
        return rdma(part, part_in.at[d], send_p.at[i], recv_p.at[d], dev(depth=to))

    def part_from(i):
        frm = (d + i) % nd
        return rdma(part, part_in.at[frm], send_p.at[i], recv_p.at[frm], dev(depth=frm))

    def sum_copy(i, j):
        return rdma(
            sums.at[here],
            sums.at[here],
            send_s.at[i * nm + j],
            recv_s.at[here],
            dev(depth=(d + i) % nd, member=(me + j) % nm),
        )

    def sum_from(i, j):
        slot = ((d + i) % nd) * nm + (me + j) % nm
        return rdma(
            sums.at[slot],
            sums.at[slot],
            send_s.at[i * nm + j],
            recv_s.at[slot],
            dev(depth=(d + i) % nd, member=(me + j) % nm),
        )

    for i, j in group:
        sum_copy(i, j).start()
    for i in range(1, nd):
        part_copy(i).start()
    send_bulk(1)

    for i, j in group:
        sum_from(i, j).wait_recv()
    mean_sum = sums[0][:1]
    for i in range(1, nd * nm):
        mean_sum = mean_sum + sums[i][:1]
    obs_mean = mean_sum / members
    predicted = part[...]
    for i in range(1, nd):
        part_from(i).wait_recv()
        predicted = predicted + part_in[(d + i) % nd]
    deviation = predicted - obs_mean
    part_in[d] = deviation
    obs[me, :, kk : 2 * kk] = deviation.astype(BF16)
    squares[me] = jnp.broadcast_to(
        jnp.sum(deviation * deviation, axis=0, keepdims=True), (8, kk)
    )

    def square_copy(j, slot):
        return rdma(
            squares.at[slot],
            squares.at[slot],
            send_q.at[j],
            recv_q.at[slot],
            dev(member=(me + j) % nm),
        )

    def obs_copy(j, slot):
        block = obs.at[slot, :, pl.ds(kk, kk)]
        return rdma(block, block, send_o.at[j], recv_o.at[slot], dev(member=(me + j) % nm))

    def side_obs(side, slot, pair, to):
        window = 2 * kk if side == 0 else 0
        return rdma(
            obs.at[slot, :, pl.ds(kk, kk)],
            obs.at[slot, :, pl.ds(window, kk)],
            send_z.at[side, pair, to],
            recv_z.at[1 - side, slot],
            dev(region=r + (2 * side - 1), member=2 * q + to),
        )

    for j in range(1, nm):
        square_copy(j, me).start()
    for j in range(1, nm):
        obs_copy(j, me).start()
    for side in (0, 1):

        @pl.when(has_side[side])
        def _():
            for to in (0, 1):
                side_obs(side, me, 0, to).start()

        @pl.when(jnp.logical_not(has_side[side]))
        def _():
            window = 0 if side == 0 else 2 * kk
            obs[:, :, window : window + kk] = jnp.zeros((nm, mm, kk), BF16)
            pert[:, :, window : window + kk] = jnp.zeros((2, mm, kk), BF16)
            stats[2 * side] = jnp.zeros((8, kk), F32)

    def send_rest(l, carry):
        send_bulk(l)
        return carry

    lax.fori_loop(2, nl, send_rest, 0)

    for j in range(1, nm):
        square_copy(j, (me + j) % nm).wait_recv()
    square_sum = squares[0][:1]
    for j in range(1, nm):
        square_sum = square_sum + squares[j][:1]
    spread = square_sum / (members - 1)
    error = errors[...]
    innovation = values[...] - obs_mean
    first = jnp.sum(innovation * innovation, axis=1, keepdims=True)
    second = jnp.sum(spread + error, axis=1, keepdims=True)
    rows = lax.broadcasted_iota(jnp.int32, (8, 128), 0)
    totals[r] = jnp.where(rows == 0, first, second)

    def total_copy(i, slot):
        return rdma(
            totals.at[slot],
            totals.at[slot],
            send_g.at[i],
            recv_g.at[slot],
            dev(region=(r + i) % nr),
        )

    for i in range(1, nr):
        total_copy(i, r).start()

    for g in range(1, ng):
        slot = 2 * ((q + g) % ng) + c
        obs_copy(2 * g, slot).wait_recv()
        for side in (0, 1):

            @pl.when(has_side[side])
            def _():
                for to in (0, 1):
                    side_obs(side, slot, g, to).start()

    for i in range(1, nr):
        total_copy(i, (r + i) % nr).wait_recv()
    grand = totals[0]
    for i in range(1, nr):
        grand = grand + totals[i]
    inflation = grand[0:1, 0:1] / grand[1:2, 0:1]
    root = jnp.sqrt(inflation)
    infl_out[...] = inflation
    factor = inflation / (inflation * spread + error)
    srow = lax.broadcasted_iota(jnp.int32, (8, kk), 0)
    stats[1] = jnp.where(srow == 0, tiles[...].astype(F32), factor / (members - 1))
    local_noise.wait()
    pert[c, :, kk : 2 * kk] = (
        innovation + jnp.sqrt(error) * noise_v[...] - root * part_in[d]
    ).astype(BF16)

    def stat_copy(side):
        return rdma(
            stats.at[1],
            stats.at[2 - 2 * side],
            send_st.at[side],
            recv_st.at[1 - side],
            dev(region=r + (2 * side - 1)),
        )

    def sib_pert(slot):
        block = pert.at[slot, :, pl.ds(kk, kk)]
        return rdma(block, block, send_ps.at[0], recv_ps.at[0], dev(member=sib))

    def side_pert(side, slot, to):
        window = 2 * kk if side == 0 else 0
        return rdma(
            pert.at[slot, :, pl.ds(kk, kk)],
            pert.at[slot, :, pl.ds(window, kk)],
            send_pz.at[side, to],
            recv_pz.at[1 - side, slot],
            dev(region=r + (2 * side - 1), member=2 * q + to),
        )

    sib_pert(c).start()
    for side in (0, 1):

        @pl.when(has_side[side])
        def _():
            stat_copy(side).start()
            for to in (0, 1):
                side_pert(side, c, to).start()

    for side in (0, 1):

        @pl.when(has_side[side])
        def _():
            rdma(
                stats.at[1], stats.at[2 * side], send_st.at[side], recv_st.at[side], dev(region=r + (2 * side - 1))
            ).wait_recv()

    lane = (lax.broadcasted_iota(jnp.int32, (kk, half), 1) + c * half).astype(F32)
    for w in range(3):
        columns = stats[w].T
        position = columns[:, 0:1] + float((w - 1) * tt)
        close = jnp.maximum(0.0, 1.0 - jnp.abs(lane - position) * (1.0 / RADIUS))
        taper[w * kk : (w + 1) * kk] = close * close * columns[:, 1:2]

    for j in range(1, nm):
        slot = (me + j) % nm
        if j % 2 == 1:
            obs_copy(j, slot).wait_recv()
    for side in (0, 1):

        @pl.when(has_side[side])
        def _():
            for slot in range(nm):
                block = obs.at[slot, :, pl.ds(2 * kk * side, kk)]
                rdma(
                    block, block, send_z.at[side, 0, 0], recv_z.at[side, slot], dev(region=r + (2 * side - 1))
                ).wait_recv()

    for w in range(3):
        for g in range(nm):
            block = obs[g, :, w * kk : (w + 1) * kk].astype(F32)
            obs_t[w * kk : (w + 1) * kk, g * mm : (g + 1) * mm] = block.T.astype(BF16)

    sib_pert(1 - c).wait_recv()
    for side in (0, 1):

        @pl.when(has_side[side])
        def _():
            for slot in (0, 1):
                block = pert.at[slot, :, pl.ds(2 * kk * side, kk)]
                rdma(
                    block, block, send_pz.at[side, 0], recv_pz.at[side, slot], dev(region=r + (2 * side - 1))
                ).wait_recv()

    local_half.wait()
    step = kk // 2

    def out_half(l, which):
        return out.at[l, :, pl.ds(pl.multiple_of(which * half, 128), half)]

    def out_local(l):
        return pltpu.make_async_copy(result.at[l, c], out_half(l, c), own_out.at[l])

    def out_remote(l):
        return rdma(
            result.at[l, 1 - c], out_half(l, c), send_out.at[l], recv_out.at[l], dev(member=sib)
        )

    def out_from(l):
        return rdma(
            result.at[l, 1 - c], out_half(l, 1 - c), send_out.at[l], recv_out.at[l], dev(member=sib)
        )

    def one_variable(l, carry):
        for j in range(1, nm):
            slot = (me + j) % nm
            rdma(
                gathered.at[l, slot],
                gathered.at[l, slot],
                send_e.at[l, j],
                recv_e.at[l, slot],
                dev(member=slot),
            ).wait_recv()
        raw = gathered[l].astype(F32)
        mean = jnp.sum(jnp.sum(raw, axis=0), axis=0, keepdims=True) / members
        anom[...] = (raw - mean[None]).astype(BF16)
        right = anom[...].reshape(members, half)

        def one_block(b, inner):
            rows_of = pl.ds(pl.multiple_of(b * step, step), step)
            cov = jnp.dot(obs_t[rows_of], right, preferred_element_type=F32)
            gain[rows_of] = (cov * taper[rows_of]).astype(BF16)
            return inner

        lax.fori_loop(0, 3 * kk // step, one_block, 0)
        increment = jnp.dot(
            pert[...].reshape(2 * mm, 3 * kk), gain[...], preferred_element_type=F32
        )
        base = mean[None] + root[None] * anom[pl.ds(2 * q, 2)].astype(F32)
        result[l] = (base + increment.reshape(2, mm, half)).astype(BF16)
        out_local(l).start()
        out_remote(l).start()
        return carry

    lax.fori_loop(0, nl, one_variable, 0)

    def finish(l, carry):
        for j in range(1, nm):
            bulk(l, j).wait_send()
        out_local(l).wait()
        out_remote(l).wait_send()
        out_from(l).wait_recv()
        return carry

    lax.fori_loop(0, nl, finish, 0)
    for i, j in group:
        sum_copy(i, j).wait_send()
    for i in range(1, nd):
        part_copy(i).wait_send()
    for j in range(1, nm):
        square_copy(j, me).wait_send()
        obs_copy(j, me).wait_send()
    for i in range(1, nr):
        total_copy(i, r).wait_send()
    sib_pert(c).wait_send()
    for side in (0, 1):

        @pl.when(has_side[side])
        def _():
            for to in (0, 1):
                side_obs(side, me, 0, to).wait_send()
                for g in range(1, ng):
                    side_obs(side, 2 * ((q + g) % ng) + c, g, to).wait_send()
                side_pert(side, c, to).wait_send()
            stat_copy(side).wait_send()


def solution(mesh):
    nr, nd, nm = (mesh.shape[a] for a in ("region", "depth", "member"))

    def shards(ensemble, obs_weights, obs_tiles, obs_values, obs_error, obs_noise):
        nl, mm, tt = ensemble.shape
        kk = obs_tiles.shape[0]
        ng = nm // 2
        half = tt // 2
        dma = pltpu.SemaphoreType.DMA
        vmem = pl.BlockSpec(memory_space=pltpu.VMEM)
        anywhere = pl.BlockSpec(memory_space=pl.ANY)
        analysis, inflation = pl.pallas_call(
            functools.partial(kernel, (nr, nd, nm, nl, mm, tt, kk)),
            out_shape=(
                jax.ShapeDtypeStruct((nl, mm, tt), BF16),
                jax.ShapeDtypeStruct((1, 1), F32),
            ),
            in_specs=[
                pl.BlockSpec(memory_space=pltpu.SMEM),
                anywhere,
                vmem,
                vmem,
                vmem,
                anywhere,
            ],
            out_specs=(anywhere, vmem),
            scratch_shapes=[
                pltpu.VMEM((nl, mm, tt), BF16),
                pltpu.VMEM((nl, nm, mm, half), BF16),
                pltpu.VMEM((mm, kk), F32),
                pltpu.VMEM((mm, kk), F32),
                pltpu.VMEM((nd, mm, kk), F32),
                pltpu.VMEM((nd * nm, 8, kk), F32),
                pltpu.VMEM((nm, 8, kk), F32),
                pltpu.VMEM((nr, 8, 128), F32),
                pltpu.VMEM((3, 8, kk), F32),
                pltpu.VMEM((nm, mm, 3 * kk), BF16),
                pltpu.VMEM((2, mm, 3 * kk), BF16),
                pltpu.VMEM((3 * kk, nm * mm), BF16),
                pltpu.VMEM((3 * kk, half), F32),
                pltpu.VMEM((nm, mm, half), BF16),
                pltpu.VMEM((3 * kk, half), BF16),
                pltpu.VMEM((nl, 2, mm, half), BF16),
                dma((3,)),
                dma((nl, nm)),
                dma((nl, nm)),
                dma((nd * nm,)),
                dma((nd * nm,)),
                dma((nd,)),
                dma((nd,)),
                dma((nm,)),
                dma((nm,)),
                dma((nm,)),
                dma((nm,)),
                dma((nr,)),
                dma((nr,)),
                dma((2, ng, 2)),
                dma((2, nm)),
                dma((2,)),
                dma((2,)),
                dma((1,)),
                dma((1,)),
                dma((2, 2)),
                dma((2, 2)),
                dma((nl,)),
                dma((nl,)),
                dma((nl,)),
            ],
            compiler_params=pltpu.CompilerParams(
                collective_id=0, has_side_effects=True, vmem_limit_bytes=56 * 1024 * 1024
            ),
        )(
            obs_weights,
            ensemble,
            obs_tiles.reshape(1, kk),
            obs_values.reshape(1, kk),
            obs_error.reshape(1, kk),
            obs_noise,
        )
        return analysis, inflation.reshape(())

    return jax.shard_map(
        shards,
        mesh=mesh,
        in_specs=(
            P("depth", "member", "region"),
            P("depth"),
            P("region"),
            P("region"),
            P("region"),
            P("member", "region"),
        ),
        out_specs=(P("depth", "member", "region"), P()),
        check_vma=False,
    )
```

```python
import functools

import jax
import jax.numpy as jnp
from jax import lax
from jax.experimental import pallas as pl
from jax.experimental.pallas import tpu as pltpu
from jax.sharding import PartitionSpec as P

RADIUS = 1024
EARLY = 1
F32 = jnp.float32
BF16 = jnp.bfloat16
MESH = pl.DeviceIdType.MESH


def kernel(
    sizes,
    weights,
    ensemble,
    tiles,
    values,
    errors,
    noise,
    out,
    infl_out,
    own,
    gathered,
    noise_v,
    part,
    part_in,
    squares,
    totals,
    stats,
    obs,
    pert,
    obs_t,
    taper,
    anom,
    means,
    gain,
    result,
    local_sem,
    send_e,
    recv_e,
    send_p,
    recv_p,
    send_q,
    recv_q,
    send_o,
    recv_o,
    send_g,
    recv_g,
    send_z,
    recv_z,
    send_st,
    recv_st,
    send_ps,
    recv_ps,
    send_pz,
    recv_pz,
    send_pf,
    recv_pf,
    send_f,
    recv_f,
    send_out,
    recv_out,
    own_out,
):
    nr, nd, nm, nl, mm, tt, kk = sizes
    ng = nm // 2
    half = tt // 2
    members = nm * mm
    r = lax.axis_index("region")
    d = lax.axis_index("depth")
    me = lax.axis_index("member")
    q = me // 2
    c = me % 2
    sib = 2 * q + (1 - c)
    has_side = (r > 0, r < nr - 1)

    def dev(region=None, depth=None, member=None):
        return {
            "region": r if region is None else region,
            "depth": d if depth is None else depth,
            "member": me if member is None else member,
        }

    def rdma(src, dst, ssem, rsem, device):
        return pltpu.make_async_remote_copy(
            src_ref=src,
            dst_ref=dst,
            send_sem=ssem,
            recv_sem=rsem,
            device_id=device,
            device_id_type=MESH,
        )

    local_own = pltpu.make_async_copy(ensemble, own, local_sem.at[0])
    local_own.start()
    local_half = pltpu.make_async_copy(
        ensemble.at[:, :, pl.ds(pl.multiple_of(c * half, 128), half)],
        gathered.at[:, me],
        local_sem.at[1],
    )
    local_half.start()
    local_noise = pltpu.make_async_copy(noise, noise_v, local_sem.at[2])
    local_noise.start()

    group = [(i, 0) for i in range(1, nd)] + [(0, j) for j in range(1, nm)]
    barrier = pltpu.get_barrier_semaphore()
    signals = 0
    for i, j in group:
        pl.semaphore_signal(
            barrier,
            inc=1,
            device_id=dev(depth=(d + i) % nd, member=(me + j) % nm),
            device_id_type=MESH,
        )
        signals += 1
    for i in range(1, nr):
        pl.semaphore_signal(
            barrier, inc=1, device_id=dev(region=(r + i) % nr), device_id_type=MESH
        )
        signals += 1
    pl.semaphore_wait(barrier, signals)

    def bulk(l, j):
        to = (me + j) % nm
        return rdma(
            ensemble.at[l, :, pl.ds(pl.multiple_of((to % 2) * half, 128), half)],
            gathered.at[l, me],
            send_e.at[l, j],
            recv_e.at[l, me],
            dev(member=to),
        )

    def send_bulk(l):
        for j in range(1, nm):
            bulk(l, j).start()

    send_bulk(0)
    local_own.wait()
    total = own[0].astype(F32) * weights[0]
    for l in range(1, nl):
        total = total + own[l].astype(F32) * weights[l]
    hi = total.astype(BF16)
    rest = total - hi.astype(F32)
    mid = rest.astype(BF16)
    low = (rest - mid.astype(F32)).astype(BF16)
    tile_ids = lax.broadcasted_iota(jnp.int32, (tt, kk), 0)
    onehot = jnp.where(tile_ids == tiles[...], 1.0, 0.0).astype(BF16)
    picked = (
        jnp.dot(hi, onehot, preferred_element_type=F32)
        + jnp.dot(mid, onehot, preferred_element_type=F32)
        + jnp.dot(low, onehot, preferred_element_type=F32)
    )
    part[...] = picked
    def part_copy(i):
        to = (d + i) % nd
        return rdma(part, part_in.at[d], send_p.at[i], recv_p.at[d], dev(depth=to))

    def part_from(i):
        frm = (d + i) % nd
        return rdma(part, part_in.at[frm], send_p.at[i], recv_p.at[frm], dev(depth=frm))

    for i in range(1, nd):
        part_copy(i).start()

    predicted = part[...]
    for i in range(1, nd):
        part_from(i).wait_recv()
        predicted = predicted + part_in[(d + i) % nd]
    own_sum = jnp.sum(predicted, axis=0, keepdims=True)
    spread_in = predicted - own_sum / mm
    own_square = jnp.sum(spread_in * spread_in, axis=0, keepdims=True)
    krow = lax.broadcasted_iota(jnp.int32, (8, kk), 0)
    squares[me] = jnp.where(krow == 0, own_sum, own_square)
    obs[me, :, kk : 2 * kk] = spread_in.astype(BF16)

    def square_copy(j, slot):
        return rdma(
            squares.at[slot],
            squares.at[slot],
            send_q.at[j],
            recv_q.at[slot],
            dev(member=(me + j) % nm),
        )

    def obs_copy(j, slot):
        block = obs.at[slot, :, pl.ds(kk, kk)]
        return rdma(block, block, send_o.at[j], recv_o.at[slot], dev(member=(me + j) % nm))

    def side_obs(side, slot, pair):
        window = 2 * kk if side == 0 else 0
        return rdma(
            obs.at[slot, :, pl.ds(kk, kk)],
            obs.at[slot, :, pl.ds(window, kk)],
            send_z.at[side, pair],
            recv_z.at[1 - side, pair],
            dev(region=r + (2 * side - 1)),
        )

    def obs_forward(w, slot, pair):
        block = obs.at[slot, :, pl.ds(w * kk, kk)]
        return rdma(block, block, send_f.at[w, pair], recv_f.at[w, pair], dev(member=sib))

    def cross(g):
        return 2 * ((q + g) % ng) + c

    def cross_sib(g):
        return 2 * ((q + g) % ng) + (1 - c)

    for j in range(1, nm):
        square_copy(j, me).start()
    for g in range(1, ng):
        obs_copy(2 * g, me).start()
    obs_forward(1, me, 0).start()
    for side in (0, 1):

        @pl.when(has_side[side])
        def _():
            side_obs(side, me, 0).start()

        @pl.when(jnp.logical_not(has_side[side]))
        def _():
            window = 0 if side == 0 else 2 * kk
            obs[:, :, window : window + kk] = jnp.zeros((nm, mm, kk), BF16)
            pert[:, :, window : window + kk] = jnp.zeros((2, mm, kk), BF16)
            stats[2 * side] = jnp.zeros((8, kk), F32)

    def send_rest(l, carry):
        send_bulk(l)
        return carry

    lax.fori_loop(1, nl, send_rest, 0)

    for j in range(1, nm):
        square_copy(j, (me + j) % nm).wait_recv()
    moments = [squares[j] for j in range(nm)]
    obs_mean = sum(m[0:1] for m in moments) / members
    deviation = predicted - obs_mean
    part_in[d] = deviation
    square_sum = sum(
        m[1:2] + mm * (m[0:1] / mm - obs_mean) * (m[0:1] / mm - obs_mean) for m in moments
    )
    spread = square_sum / (members - 1)
    error = errors[...]
    innovation = values[...] - obs_mean
    first = jnp.sum(innovation * innovation, axis=1, keepdims=True)
    second = jnp.sum(spread + error, axis=1, keepdims=True)
    rows = lax.broadcasted_iota(jnp.int32, (8, 128), 0)
    totals[r] = jnp.where(rows == 0, first, second)

    def total_copy(i, slot):
        return rdma(
            totals.at[slot],
            totals.at[slot],
            send_g.at[i],
            recv_g.at[slot],
            dev(region=(r + i) % nr),
        )

    for i in range(1, nr):
        total_copy(i, r).start()

    for g in range(1, ng):
        obs_copy(2 * g, cross(g)).wait_recv()
        for side in (0, 1):

            @pl.when(has_side[side])
            def _():
                side_obs(side, cross(g), g).start()

        obs_forward(1, cross(g), g).start()

    for i in range(1, nr):
        total_copy(i, (r + i) % nr).wait_recv()
    grand = totals[0]
    for i in range(1, nr):
        grand = grand + totals[i]
    inflation = grand[0:1, 0:1] / grand[1:2, 0:1]
    root = jnp.sqrt(inflation)
    infl_out[...] = inflation
    factor = inflation / (inflation * spread + error)
    facts = jnp.where(krow == 0, tiles[...].astype(F32), factor / (members - 1))
    for g in range(nm):
        facts = jnp.where(krow == 2 + g, moments[g][0:1] / mm - obs_mean, facts)
    stats[1] = facts
    local_noise.wait()
    pert[c, :, kk : 2 * kk] = (
        innovation + jnp.sqrt(error) * noise_v[...] - root * part_in[d]
    ).astype(BF16)

    def stat_copy(side):
        return rdma(
            stats.at[1],
            stats.at[2 - 2 * side],
            send_st.at[side],
            recv_st.at[1 - side],
            dev(region=r + (2 * side - 1)),
        )

    def sib_pert(slot):
        block = pert.at[slot, :, pl.ds(kk, kk)]
        return rdma(block, block, send_ps.at[0], recv_ps.at[0], dev(member=sib))

    def side_pert(side):
        window = 2 * kk if side == 0 else 0
        return rdma(
            pert.at[c, :, pl.ds(kk, kk)],
            pert.at[c, :, pl.ds(window, kk)],
            send_pz.at[side],
            recv_pz.at[1 - side],
            dev(region=r + (2 * side - 1)),
        )

    def pert_forward(side, slot):
        block = pert.at[slot, :, pl.ds(2 * kk * side, kk)]
        return rdma(block, block, send_pf.at[side], recv_pf.at[side], dev(member=sib))

    sib_pert(c).start()
    for side in (0, 1):

        @pl.when(has_side[side])
        def _():
            stat_copy(side).start()
            side_pert(side).start()

    lane = (lax.broadcasted_iota(jnp.int32, (kk, half), 1) + c * half).astype(F32)

    def make_taper(w):
        columns = stats[w].T
        position = columns[:, 0:1] + float((w - 1) * tt)
        close = jnp.maximum(0.0, 1.0 - jnp.abs(lane - position) * (1.0 / RADIUS))
        taper[w * kk : (w + 1) * kk] = close * close * columns[:, 1:2]

    def transpose_all(w):
        shifts = stats[w].T
        for g in range(nm):
            block = obs[g, :, w * kk : (w + 1) * kk].astype(F32).T + shifts[:, 2 + g : 3 + g]
            obs_t[w * kk : (w + 1) * kk, g * mm : (g + 1) * mm] = block.astype(BF16)

    step = kk // 2

    def gain_blocks(l, lo, hi):
        right = anom[l].reshape(members, half)

        def one_block(b, inner):
            at = (b + 2 * (b // 2)) if lo == 0 else b
            rows_of = pl.ds(pl.multiple_of(at * step, step), step)
            cov = jnp.dot(obs_t[rows_of], right, preferred_element_type=F32)
            gain[l, rows_of] = (cov * taper[rows_of]).astype(BF16)
            return inner

        lax.fori_loop(lo, hi, one_block, 0)

    def own_window(l, carry):
        for j in range(1, nm):
            slot = (me + j) % nm
            rdma(
                gathered.at[l, slot],
                gathered.at[l, slot],
                send_e.at[l, j],
                recv_e.at[l, slot],
                dev(member=slot),
            ).wait_recv()
        raw = gathered[l].astype(F32)
        mean = jnp.sum(jnp.sum(raw, axis=0), axis=0, keepdims=True) / members
        means[l] = jnp.broadcast_to(mean, (8, half))
        anom[l] = (raw - mean[None]).astype(BF16)
        gain_blocks(l, 2, 4)
        return carry

    make_taper(1)
    for g in range(ng):
        obs_forward(1, cross_sib(g), g).wait_recv()
    transpose_all(1)
    local_half.wait()
    early = min(EARLY, nl)
    own_window(0, 0)

    for g in range(ng):
        for side in (0, 1):

            @pl.when(has_side[side])
            def _():
                side_obs(1 - side, cross(g), g).wait_recv()
                obs_forward(2 * side, cross(g), g).start()

    lax.fori_loop(1, early, own_window, 0)
    for side in (0, 1):

        @pl.when(has_side[side])
        def _():
            rdma(
                stats.at[1],
                stats.at[2 * side],
                send_st.at[side],
                recv_st.at[side],
                dev(region=r + (2 * side - 1)),
            ).wait_recv()

        make_taper(2 * side)

    for side in (0, 1):

        @pl.when(has_side[side])
        def _():
            for g in range(ng):
                obs_forward(2 * side, cross_sib(g), g).wait_recv()

        transpose_all(2 * side)

    for side in (0, 1):

        @pl.when(has_side[side])
        def _():
            side_pert(1 - side).wait_recv()
            pert_forward(side, c).start()


    def out_half(l, which):
        return out.at[l, :, pl.ds(pl.multiple_of(which * half, 128), half)]

    def out_local(l):
        return pltpu.make_async_copy(result.at[l, c], out_half(l, c), own_out.at[l])

    def out_remote(l):
        return rdma(
            result.at[l, 1 - c], out_half(l, c), send_out.at[l], recv_out.at[l], dev(member=sib)
        )

    def out_from(l):
        return rdma(
            result.at[l, 1 - c], out_half(l, 1 - c), send_out.at[l], recv_out.at[l], dev(member=sib)
        )

    def one_variable(l, carry):
        @pl.when(l >= early)
        def _():
            own_window(l, 0)

        gain_blocks(l, 0, 4)

        @pl.when(l == 0)
        def _():
            sib_pert(1 - c).wait_recv()
            for side in (0, 1):

                @pl.when(has_side[side])
                def _():
                    pert_forward(side, 1 - c).wait_recv()

        increment = jnp.dot(
            pert[...].reshape(2 * mm, 3 * kk), gain[l], preferred_element_type=F32
        )
        base = means[l][0:1][None] + root[None] * anom[l, pl.ds(2 * q, 2)].astype(F32)
        result[l] = (base + increment.reshape(2, mm, half)).astype(BF16)
        out_local(l).start()
        out_remote(l).start()
        return carry

    lax.fori_loop(0, nl, one_variable, 0)

    def finish(l, carry):
        for j in range(1, nm):
            bulk(l, j).wait_send()
        out_local(l).wait()
        out_remote(l).wait_send()
        out_from(l).wait_recv()
        return carry

    lax.fori_loop(0, nl, finish, 0)
    for i in range(1, nd):
        part_copy(i).wait_send()
    for j in range(1, nm):
        square_copy(j, me).wait_send()
    for g in range(1, ng):
        obs_copy(2 * g, me).wait_send()
    for g in range(ng):
        obs_forward(1, cross(g), g).wait_send()
    for i in range(1, nr):
        total_copy(i, r).wait_send()
    sib_pert(c).wait_send()
    for side in (0, 1):

        @pl.when(has_side[side])
        def _():
            for g in range(ng):
                side_obs(side, cross(g), g).wait_send()
                obs_forward(2 * side, cross(g), g).wait_send()
            side_pert(side).wait_send()
            pert_forward(side, c).wait_send()
            stat_copy(side).wait_send()


def hand_on(block, out):
    pass


def solution(mesh):
    nr, nd, nm = (mesh.shape[a] for a in ("region", "depth", "member"))

    def shards(ensemble, obs_weights, obs_tiles, obs_values, obs_error, obs_noise):
        nl, mm, tt = ensemble.shape
        kk = obs_tiles.shape[0]
        ng = nm // 2
        half = tt // 2
        dma = pltpu.SemaphoreType.DMA
        vmem = pl.BlockSpec(memory_space=pltpu.VMEM)
        anywhere = pl.BlockSpec(memory_space=pl.ANY)
        analysis, inflation = pl.pallas_call(
            functools.partial(kernel, (nr, nd, nm, nl, mm, tt, kk)),
            out_shape=(
                pltpu.VMEM((nl, mm, tt), BF16),
                jax.ShapeDtypeStruct((1, 1), F32),
            ),
            in_specs=[
                pl.BlockSpec(memory_space=pltpu.SMEM),
                anywhere,
                vmem,
                vmem,
                vmem,
                anywhere,
            ],
            out_specs=(vmem, vmem),
            scratch_shapes=[
                pltpu.VMEM((nl, mm, tt), BF16),
                pltpu.VMEM((nl, nm, mm, half), BF16),
                pltpu.VMEM((mm, kk), F32),
                pltpu.VMEM((mm, kk), F32),
                pltpu.VMEM((nd, mm, kk), F32),
                pltpu.VMEM((nm, 8, kk), F32),
                pltpu.VMEM((nr, 8, 128), F32),
                pltpu.VMEM((3, 8, kk), F32),
                pltpu.VMEM((nm, mm, 3 * kk), BF16),
                pltpu.VMEM((2, mm, 3 * kk), BF16),
                pltpu.VMEM((3 * kk, nm * mm), BF16),
                pltpu.VMEM((3 * kk, half), F32),
                pltpu.VMEM((nl, nm, mm, half), BF16),
                pltpu.VMEM((nl, 8, half), F32),
                pltpu.VMEM((nl, 3 * kk, half), BF16),
                pltpu.VMEM((nl, 2, mm, half), BF16),
                dma((3,)),
                dma((nl, nm)),
                dma((nl, nm)),
                dma((nd,)),
                dma((nd,)),
                dma((nm,)),
                dma((nm,)),
                dma((nm,)),
                dma((nm,)),
                dma((nr,)),
                dma((nr,)),
                dma((2, ng)),
                dma((2, ng)),
                dma((2,)),
                dma((2,)),
                dma((1,)),
                dma((1,)),
                dma((2,)),
                dma((2,)),
                dma((2,)),
                dma((2,)),
                dma((3, ng)),
                dma((3, ng)),
                dma((nl,)),
                dma((nl,)),
                dma((nl,)),
            ],
            compiler_params=pltpu.CompilerParams(
                collective_id=0, has_side_effects=True, vmem_limit_bytes=56 * 1024 * 1024
            ),
        )(
            obs_weights,
            ensemble,
            obs_tiles.reshape(1, kk),
            obs_values.reshape(1, kk),
            obs_error.reshape(1, kk),
            obs_noise,
        )
        analysis = pl.pallas_call(
            hand_on,
            out_shape=jax.ShapeDtypeStruct((nl, mm, tt), BF16),
            in_specs=[anywhere],
            out_specs=anywhere,
            input_output_aliases={0: 0},
        )(analysis)
        return analysis, inflation.reshape(())

    return jax.shard_map(
        shards,
        mesh=mesh,
        in_specs=(
            P("depth", "member", "region"),
            P("depth"),
            P("region"),
            P("region"),
            P("region"),
            P("member", "region"),
        ),
        out_specs=(P("depth", "member", "region"), P()),
        check_vma=False,
    )
```

```python
import functools

import jax
import jax.numpy as jnp
from jax import lax
from jax.experimental import pallas as pl
from jax.experimental.pallas import tpu as pltpu
from jax.sharding import PartitionSpec as P

RADIUS = 1024
EARLY = 2
F32 = jnp.float32
BF16 = jnp.bfloat16
MESH = pl.DeviceIdType.MESH


def kernel(
    sizes,
    weights,
    ensemble,
    tiles,
    values,
    errors,
    noise,
    out,
    infl_out,
    own,
    gathered,
    noise_v,
    part,
    part_in,
    squares,
    totals,
    stats,
    obs,
    pert,
    obs_t,
    taper,
    anom,
    means,
    gain,
    result,
    local_sem,
    send_e,
    recv_e,
    send_p,
    recv_p,
    send_q,
    recv_q,
    send_o,
    recv_o,
    send_g,
    recv_g,
    send_z,
    recv_z,
    send_st,
    recv_st,
    send_ps,
    recv_ps,
    send_pz,
    recv_pz,
    send_pf,
    recv_pf,
    send_f,
    recv_f,
    send_out,
    recv_out,
    own_out,
):
    nr, nd, nm, nl, mm, tt, kk = sizes
    ng = nm // 2
    half = tt // 2
    members = nm * mm
    r = lax.axis_index("region")
    d = lax.axis_index("depth")
    me = lax.axis_index("member")
    q = me // 2
    c = me % 2
    sib = 2 * q + (1 - c)
    has_side = (r > 0, r < nr - 1)

    def dev(region=None, depth=None, member=None):
        return {
            "region": r if region is None else region,
            "depth": d if depth is None else depth,
            "member": me if member is None else member,
        }

    def rdma(src, dst, ssem, rsem, device):
        return pltpu.make_async_remote_copy(
            src_ref=src,
            dst_ref=dst,
            send_sem=ssem,
            recv_sem=rsem,
            device_id=device,
            device_id_type=MESH,
        )

    local_own = pltpu.make_async_copy(ensemble, own, local_sem.at[0])
    local_own.start()
    local_half = pltpu.make_async_copy(
        ensemble.at[:, :, pl.ds(pl.multiple_of(c * half, 128), half)],
        gathered.at[:, me],
        local_sem.at[1],
    )
    local_half.start()
    local_noise = pltpu.make_async_copy(noise, noise_v, local_sem.at[2])
    local_noise.start()

    group = [(i, 0) for i in range(1, nd)] + [(0, j) for j in range(1, nm)]
    barrier = pltpu.get_barrier_semaphore()
    signals = 0
    for i, j in group:
        pl.semaphore_signal(
            barrier,
            inc=1,
            device_id=dev(depth=(d + i) % nd, member=(me + j) % nm),
            device_id_type=MESH,
        )
        signals += 1
    for i in range(1, nr):
        pl.semaphore_signal(
            barrier, inc=1, device_id=dev(region=(r + i) % nr), device_id_type=MESH
        )
        signals += 1
    pl.semaphore_wait(barrier, signals)

    def bulk(l, j):
        to = (me + j) % nm
        return rdma(
            ensemble.at[l, :, pl.ds(pl.multiple_of((to % 2) * half, 128), half)],
            gathered.at[l, me],
            send_e.at[l, j],
            recv_e.at[l, me],
            dev(member=to),
        )

    def send_bulk(l):
        for j in range(1, nm):
            bulk(l, j).start()

    send_bulk(0)
    local_own.wait()
    total = own[0].astype(F32) * weights[0]
    for l in range(1, nl):
        total = total + own[l].astype(F32) * weights[l]
    hi = total.astype(BF16)
    rest = total - hi.astype(F32)
    mid = rest.astype(BF16)
    low = (rest - mid.astype(F32)).astype(BF16)
    tile_ids = lax.broadcasted_iota(jnp.int32, (tt, kk), 0)
    onehot = jnp.where(tile_ids == tiles[...], 1.0, 0.0).astype(BF16)
    picked = (
        jnp.dot(hi, onehot, preferred_element_type=F32)
        + jnp.dot(mid, onehot, preferred_element_type=F32)
        + jnp.dot(low, onehot, preferred_element_type=F32)
    )
    part_mean = jnp.sum(picked, axis=0, keepdims=True) / mm
    top = part_mean.astype(BF16).astype(F32)
    second_row = (part_mean - top).astype(BF16).astype(F32)
    third_row = part_mean - top - second_row
    prow = lax.broadcasted_iota(jnp.int32, (16, kk), 0)
    split = jnp.where(prow == 0, top, jnp.where(prow == 1, second_row, third_row))
    part[0:mm] = (picked - part_mean).astype(BF16)
    part[mm : mm + 16] = jnp.where(prow < 3, split, 0.0).astype(BF16)

    def whole(block):
        values_of = block.astype(F32)
        return values_of[0:mm] + jnp.sum(values_of[mm : mm + 16], axis=0, keepdims=True)

    def part_copy(i):
        to = (d + i) % nd
        return rdma(part, part_in.at[d], send_p.at[i], recv_p.at[d], dev(depth=to))

    def part_from(i):
        frm = (d + i) % nd
        return rdma(part, part_in.at[frm], send_p.at[i], recv_p.at[frm], dev(depth=frm))

    for i in range(1, nd):
        part_copy(i).start()

    predicted = whole(part[...])
    for i in range(1, nd):
        part_from(i).wait_recv()
        predicted = predicted + whole(part_in[(d + i) % nd])
    own_sum = jnp.sum(predicted, axis=0, keepdims=True)
    spread_in = predicted - own_sum / mm
    own_square = jnp.sum(spread_in * spread_in, axis=0, keepdims=True)
    krow = lax.broadcasted_iota(jnp.int32, (8, kk), 0)
    squares[me] = jnp.where(krow == 0, own_sum, own_square)
    obs[me, :, kk : 2 * kk] = spread_in.astype(BF16)

    def square_copy(j, slot):
        return rdma(
            squares.at[slot],
            squares.at[slot],
            send_q.at[j],
            recv_q.at[slot],
            dev(member=(me + j) % nm),
        )

    def obs_copy(j, slot):
        block = obs.at[slot, :, pl.ds(kk, kk)]
        return rdma(block, block, send_o.at[j], recv_o.at[slot], dev(member=(me + j) % nm))

    def side_obs(side, slot, pair):
        window = 2 * kk if side == 0 else 0
        return rdma(
            obs.at[slot, :, pl.ds(kk, kk)],
            obs.at[slot, :, pl.ds(window, kk)],
            send_z.at[side, pair],
            recv_z.at[1 - side, pair],
            dev(region=r + (2 * side - 1)),
        )

    def obs_forward(w, slot, pair):
        block = obs.at[slot, :, pl.ds(w * kk, kk)]
        return rdma(block, block, send_f.at[w, pair], recv_f.at[w, pair], dev(member=sib))

    def cross(g):
        return 2 * ((q + g) % ng) + c

    def cross_sib(g):
        return 2 * ((q + g) % ng) + (1 - c)

    for j in range(1, nm):
        square_copy(j, me).start()
    for g in range(1, ng):
        obs_copy(2 * g, me).start()
    obs_forward(1, me, 0).start()
    for side in (0, 1):

        @pl.when(has_side[side])
        def _():
            side_obs(side, me, 0).start()

        @pl.when(jnp.logical_not(has_side[side]))
        def _():
            window = 0 if side == 0 else 2 * kk
            obs[:, :, window : window + kk] = jnp.zeros((nm, mm, kk), BF16)
            pert[:, :, window : window + kk] = jnp.zeros((2, mm, kk), BF16)
            stats[2 * side] = jnp.zeros((8, kk), F32)

    def send_rest(l, carry):
        send_bulk(l)
        return carry

    lax.fori_loop(1, nl, send_rest, 0)

    for j in range(1, nm):
        square_copy(j, (me + j) % nm).wait_recv()
    moments = [squares[j] for j in range(nm)]
    obs_mean = sum(m[0:1] for m in moments) / members
    deviation = predicted - obs_mean
    square_sum = sum(
        m[1:2] + mm * (m[0:1] / mm - obs_mean) * (m[0:1] / mm - obs_mean) for m in moments
    )
    spread = square_sum / (members - 1)
    error = errors[...]
    innovation = values[...] - obs_mean
    first = jnp.sum(innovation * innovation, axis=1, keepdims=True)
    second = jnp.sum(spread + error, axis=1, keepdims=True)
    rows = lax.broadcasted_iota(jnp.int32, (8, 128), 0)
    totals[r] = jnp.where(rows == 0, first, second)

    def total_copy(i, slot):
        return rdma(
            totals.at[slot],
            totals.at[slot],
            send_g.at[i],
            recv_g.at[slot],
            dev(region=(r + i) % nr),
        )

    for i in range(1, nr):
        total_copy(i, r).start()

    for g in range(1, ng):
        obs_copy(2 * g, cross(g)).wait_recv()
        for side in (0, 1):

            @pl.when(has_side[side])
            def _():
                side_obs(side, cross(g), g).start()

        obs_forward(1, cross(g), g).start()

    for i in range(1, nr):
        total_copy(i, (r + i) % nr).wait_recv()
    grand = totals[0]
    for i in range(1, nr):
        grand = grand + totals[i]
    inflation = grand[0:1, 0:1] / grand[1:2, 0:1]
    root = jnp.sqrt(inflation)
    infl_out[...] = inflation
    factor = inflation / (inflation * spread + error)
    facts = jnp.where(krow == 0, tiles[...].astype(F32), factor / (members - 1))
    for g in range(nm):
        facts = jnp.where(krow == 2 + g, moments[g][0:1] / mm - obs_mean, facts)
    stats[1] = facts
    local_noise.wait()
    pert[c, :, kk : 2 * kk] = (
        innovation + jnp.sqrt(error) * noise_v[...] - root * deviation
    ).astype(BF16)

    def stat_copy(side):
        return rdma(
            stats.at[1],
            stats.at[2 - 2 * side],
            send_st.at[side],
            recv_st.at[1 - side],
            dev(region=r + (2 * side - 1)),
        )

    def sib_pert(slot):
        block = pert.at[slot, :, pl.ds(kk, kk)]
        return rdma(block, block, send_ps.at[0], recv_ps.at[0], dev(member=sib))

    def side_pert(side):
        window = 2 * kk if side == 0 else 0
        return rdma(
            pert.at[c, :, pl.ds(kk, kk)],
            pert.at[c, :, pl.ds(window, kk)],
            send_pz.at[side],
            recv_pz.at[1 - side],
            dev(region=r + (2 * side - 1)),
        )

    def pert_forward(side, slot):
        block = pert.at[slot, :, pl.ds(2 * kk * side, kk)]
        return rdma(block, block, send_pf.at[side], recv_pf.at[side], dev(member=sib))

    sib_pert(c).start()
    for side in (0, 1):

        @pl.when(has_side[side])
        def _():
            stat_copy(side).start()
            side_pert(side).start()

    lane = (lax.broadcasted_iota(jnp.int32, (kk, half), 1) + c * half).astype(F32)

    def make_taper(w):
        columns = stats[w].T
        position = columns[:, 0:1] + float((w - 1) * tt)
        close = jnp.maximum(0.0, 1.0 - jnp.abs(lane - position) * (1.0 / RADIUS))
        taper[w * kk : (w + 1) * kk] = close * close * columns[:, 1:2]

    def transpose_all(w):
        shifts = stats[w].T
        for g in range(nm):
            block = obs[g, :, w * kk : (w + 1) * kk].astype(F32).T + shifts[:, 2 + g : 3 + g]
            obs_t[w * kk : (w + 1) * kk, g * mm : (g + 1) * mm] = block.astype(BF16)

    step = kk // 2

    def gain_blocks(l, lo, hi):
        right = anom[l].reshape(members, half)

        def one_block(b, inner):
            at = (b + 2 * (b // 2)) if lo == 0 else b
            rows_of = pl.ds(pl.multiple_of(at * step, step), step)
            cov = jnp.dot(obs_t[rows_of], right, preferred_element_type=F32)
            gain[l, rows_of] = (cov * taper[rows_of]).astype(BF16)
            return inner

        lax.fori_loop(lo, hi, one_block, 0)

    def own_window(l, carry):
        for j in range(1, nm):
            slot = (me + j) % nm
            rdma(
                gathered.at[l, slot],
                gathered.at[l, slot],
                send_e.at[l, j],
                recv_e.at[l, slot],
                dev(member=slot),
            ).wait_recv()
        raw = gathered[l].astype(F32)
        mean = jnp.sum(jnp.sum(raw, axis=0), axis=0, keepdims=True) / members
        means[l] = jnp.broadcast_to(mean, (8, half))
        anom[l] = (raw - mean[None]).astype(BF16)
        gain_blocks(l, 2, 4)
        return carry

    make_taper(1)
    for g in range(ng):
        obs_forward(1, cross_sib(g), g).wait_recv()
    transpose_all(1)
    local_half.wait()
    early = min(EARLY, nl)
    own_window(0, 0)

    for g in range(ng):
        for side in (0, 1):

            @pl.when(has_side[side])
            def _():
                side_obs(1 - side, cross(g), g).wait_recv()
                obs_forward(2 * side, cross(g), g).start()

    for side in (0, 1):

        @pl.when(has_side[side])
        def _():
            rdma(
                stats.at[1],
                stats.at[2 * side],
                send_st.at[side],
                recv_st.at[side],
                dev(region=r + (2 * side - 1)),
            ).wait_recv()

        make_taper(2 * side)

    for side in (0, 1):

        @pl.when(has_side[side])
        def _():
            for g in range(ng):
                obs_forward(2 * side, cross_sib(g), g).wait_recv()

        transpose_all(2 * side)

    def out_half(l, which):
        return out.at[l, :, pl.ds(pl.multiple_of(which * half, 128), half)]

    def out_local(l):
        return pltpu.make_async_copy(result.at[l, c], out_half(l, c), own_out.at[l])

    def out_remote(l):
        return rdma(
            result.at[l, 1 - c], out_half(l, c), send_out.at[l], recv_out.at[l], dev(member=sib)
        )

    def out_from(l):
        return rdma(
            result.at[l, 1 - c], out_half(l, 1 - c), send_out.at[l], recv_out.at[l], dev(member=sib)
        )

    def one_variable(l, carry):
        @pl.when(l >= early)
        def _():
            own_window(l, 0)

        gain_blocks(l, 0, 4)

        @pl.when(l == 0)
        def _():
            for side in (0, 1):

                @pl.when(has_side[side])
                def _():
                    side_pert(1 - side).wait_recv()
                    pert_forward(side, c).start()

            for ahead in range(1, early):
                own_window(ahead, 0)
            sib_pert(1 - c).wait_recv()
            for side in (0, 1):

                @pl.when(has_side[side])
                def _():
                    pert_forward(side, 1 - c).wait_recv()

        increment = jnp.dot(
            pert[...].reshape(2 * mm, 3 * kk), gain[l], preferred_element_type=F32
        )
        base = means[l][0:1][None] + root[None] * anom[l, pl.ds(2 * q, 2)].astype(F32)
        result[l] = (base + increment.reshape(2, mm, half)).astype(BF16)
        out_local(l).start()
        out_remote(l).start()
        return carry

    lax.fori_loop(0, nl, one_variable, 0)

    def finish(l, carry):
        for j in range(1, nm):
            bulk(l, j).wait_send()
        out_local(l).wait()
        out_remote(l).wait_send()
        out_from(l).wait_recv()
        return carry

    lax.fori_loop(0, nl, finish, 0)
    for i in range(1, nd):
        part_copy(i).wait_send()
    for j in range(1, nm):
        square_copy(j, me).wait_send()
    for g in range(1, ng):
        obs_copy(2 * g, me).wait_send()
    for g in range(ng):
        obs_forward(1, cross(g), g).wait_send()
    for i in range(1, nr):
        total_copy(i, r).wait_send()
    sib_pert(c).wait_send()
    for side in (0, 1):

        @pl.when(has_side[side])
        def _():
            for g in range(ng):
                side_obs(side, cross(g), g).wait_send()
                obs_forward(2 * side, cross(g), g).wait_send()
            side_pert(side).wait_send()
            pert_forward(side, c).wait_send()
            stat_copy(side).wait_send()


def hand_on(block, out):
    pass


def solution(mesh):
    nr, nd, nm = (mesh.shape[a] for a in ("region", "depth", "member"))

    def shards(ensemble, obs_weights, obs_tiles, obs_values, obs_error, obs_noise):
        nl, mm, tt = ensemble.shape
        kk = obs_tiles.shape[0]
        ng = nm // 2
        half = tt // 2
        dma = pltpu.SemaphoreType.DMA
        vmem = pl.BlockSpec(memory_space=pltpu.VMEM)
        anywhere = pl.BlockSpec(memory_space=pl.ANY)
        analysis, inflation = pl.pallas_call(
            functools.partial(kernel, (nr, nd, nm, nl, mm, tt, kk)),
            out_shape=(
                pltpu.VMEM((nl, mm, tt), BF16),
                jax.ShapeDtypeStruct((1, 1), F32),
            ),
            in_specs=[
                pl.BlockSpec(memory_space=pltpu.SMEM),
                anywhere,
                vmem,
                vmem,
                vmem,
                anywhere,
            ],
            out_specs=(vmem, vmem),
            scratch_shapes=[
                pltpu.VMEM((nl, mm, tt), BF16),
                pltpu.VMEM((nl, nm, mm, half), BF16),
                pltpu.VMEM((mm, kk), F32),
                pltpu.VMEM((mm + 16, kk), BF16),
                pltpu.VMEM((nd, mm + 16, kk), BF16),
                pltpu.VMEM((nm, 8, kk), F32),
                pltpu.VMEM((nr, 8, 128), F32),
                pltpu.VMEM((3, 8, kk), F32),
                pltpu.VMEM((nm, mm, 3 * kk), BF16),
                pltpu.VMEM((2, mm, 3 * kk), BF16),
                pltpu.VMEM((3 * kk, nm * mm), BF16),
                pltpu.VMEM((3 * kk, half), F32),
                pltpu.VMEM((nl, nm, mm, half), BF16),
                pltpu.VMEM((nl, 8, half), F32),
                pltpu.VMEM((nl, 3 * kk, half), BF16),
                pltpu.VMEM((nl, 2, mm, half), BF16),
                dma((3,)),
                dma((nl, nm)),
                dma((nl, nm)),
                dma((nd,)),
                dma((nd,)),
                dma((nm,)),
                dma((nm,)),
                dma((nm,)),
                dma((nm,)),
                dma((nr,)),
                dma((nr,)),
                dma((2, ng)),
                dma((2, ng)),
                dma((2,)),
                dma((2,)),
                dma((1,)),
                dma((1,)),
                dma((2,)),
                dma((2,)),
                dma((2,)),
                dma((2,)),
                dma((3, ng)),
                dma((3, ng)),
                dma((nl,)),
                dma((nl,)),
                dma((nl,)),
            ],
            compiler_params=pltpu.CompilerParams(
                collective_id=0, has_side_effects=True, vmem_limit_bytes=56 * 1024 * 1024
            ),
        )(
            obs_weights,
            ensemble,
            obs_tiles.reshape(1, kk),
            obs_values.reshape(1, kk),
            obs_error.reshape(1, kk),
            obs_noise,
        )
        analysis = pl.pallas_call(
            hand_on,
            out_shape=jax.ShapeDtypeStruct((nl, mm, tt), BF16),
            in_specs=[anywhere],
            out_specs=anywhere,
            input_output_aliases={0: 0},
        )(analysis)
        return analysis, inflation.reshape(())

    return jax.shard_map(
        shards,
        mesh=mesh,
        in_specs=(
            P("depth", "member", "region"),
            P("depth"),
            P("region"),
            P("region"),
            P("region"),
            P("member", "region"),
        ),
        out_specs=(P("depth", "member", "region"), P()),
        check_vma=False,
    )
```
